8 devices in a mesh: dp: 2 (over z, y), cp: 4 (over x, core).
Axes of the slice: x: 2, y: 2, z: 1, core: 2. Of those that a mesh axis runs over, the one named last changes fastest.
Arguments:
- x_in: bfloat16 [6, 2048, 1536], P('dp', 'cp')
- d_out: bfloat16 [6, 2048, 1536], P('dp', 'cp')
- w_q: bfloat16 [1536, 12, 128], replicated
- w_k: bfloat16 [1536, 12, 128], replicated
- w_v: bfloat16 [1536, 12, 128], replicated
- w_o: bfloat16 [12, 128, 1536], replicated
- w_up: bfloat16 [1536, 8960], replicated
- w_down: bfloat16 [8960, 1536], replicated
Outputs:
- output 1: bfloat16 [6, 2048, 1536], P('dp', 'cp')
- output 2: float32 [1536, 12, 128], replicated
- output 3: float32 [1536, 12, 128], replicated
- output 4: float32 [1536, 12, 128], replicated
- output 5: float32 [12, 128, 1536], replicated
- output 6: float32 [1536, 8960], replicated
- output 7: float32 [8960, 1536], replicated
All inputs are finite; a program needn't handle non-finite values.
Results may differ from the reference program's by a relative error of at most 0.0183747.
Values are sent between devices in bfloat16 or wider.
A program may use at most 1 GiB of HBM per device.

```python
import jax
import jax.numpy as jnp
from jax import lax

BATCH_SIZE = 6
SEQ_LEN = 2048
D_MODEL = 1536
N_HEADS = 12
HEAD_DIM = 128
FFN_DIM = 8960
N_SHARDS = 8
Q_BLOCK = 256


def setup_inputs(seed: int = 0) -> dict:
    key_list = jax.random.split(jax.random.key(seed), 8)
    attn_width = N_HEADS * HEAD_DIM
    act_shape = (BATCH_SIZE, SEQ_LEN, D_MODEL)

    def draw_normal(key_part, arr_shape, std_dev):
        return (jax.random.normal(key_part, arr_shape, jnp.float32) * std_dev).astype(jnp.bfloat16)

    return {
        'x_in': draw_normal(key_list[0], act_shape, 1.0),
        'd_out': draw_normal(key_list[1], act_shape, 1.0),
        'w_q': draw_normal(key_list[2], (D_MODEL, N_HEADS, HEAD_DIM), D_MODEL ** -0.5),
        'w_k': draw_normal(key_list[3], (D_MODEL, N_HEADS, HEAD_DIM), D_MODEL ** -0.5),
        'w_v': draw_normal(key_list[4], (D_MODEL, N_HEADS, HEAD_DIM), D_MODEL ** -0.5),
        'w_o': draw_normal(key_list[5], (N_HEADS, HEAD_DIM, D_MODEL), attn_width ** -0.5),
        'w_up': draw_normal(key_list[6], (D_MODEL, FFN_DIM), D_MODEL ** -0.5),
        'w_down': draw_normal(key_list[7], (FFN_DIM, D_MODEL), FFN_DIM ** -0.5),
    }


def keep_bf16(values):
    return values.astype(jnp.bfloat16).astype(jnp.float32)


def stored_positions():
    n_blocks = SEQ_LEN // Q_BLOCK
    stored = jnp.arange(n_blocks)
    owner_rank = stored // 2
    seq_block = owner_rank + (stored % 2) * (n_blocks - 1 - 2 * owner_rank)
    return (seq_block[:, None] * Q_BLOCK + jnp.arange(Q_BLOCK)[None, :]).reshape(SEQ_LEN)


def attend_block(q_rows, pos_rows, key_seq, val_seq, positions):
    scores = jnp.einsum('qhe,khe->hqk', q_rows, key_seq) * (HEAD_DIM ** -0.5)
    scores = jnp.where(positions[None, None, :] <= pos_rows[None, :, None], scores, -1e30)
    prob_b = keep_bf16(jax.nn.softmax(scores, axis=-1))
    return keep_bf16(jnp.einsum('hqk,khe->qhe', prob_b, val_seq))


def attend_sequence(q_seq, key_seq, val_seq, positions):
    n_blocks = SEQ_LEN // Q_BLOCK
    q_blocks = q_seq.reshape(n_blocks, Q_BLOCK, N_HEADS, HEAD_DIM)
    pos_blocks = positions.reshape(n_blocks, Q_BLOCK)
    block_fn = jax.checkpoint(attend_block)
    outs = lax.map(lambda block_pair: block_fn(block_pair[0], block_pair[1], key_seq, val_seq, positions), (q_blocks, pos_blocks))
    return outs.reshape(SEQ_LEN, N_HEADS, HEAD_DIM)


def reference(x_in, d_out, w_q, w_k, w_v, w_o, w_up, w_down):
    positions = stored_positions()

    def forward(x_f32, wq_f32, wk_f32, wv_f32, wo_f32, wu_f32, wd_f32):
        q_seq = keep_bf16(jnp.einsum('bsd,dhe->bshe', x_f32, wq_f32))
        k_seq = keep_bf16(jnp.einsum('bsd,dhe->bshe', x_f32, wk_f32))
        v_seq = keep_bf16(jnp.einsum('bsd,dhe->bshe', x_f32, wv_f32))
        attn_out = lax.map(lambda qkv_rows: attend_sequence(qkv_rows[0], qkv_rows[1], qkv_rows[2], positions), (q_seq, k_seq, v_seq))
        hidden = keep_bf16(x_f32 + jnp.einsum('bshe,hed->bsd', attn_out, wo_f32))
        up_pre = keep_bf16(jnp.einsum('bsd,df->bsf', hidden, wu_f32))
        act_val = keep_bf16(jax.nn.gelu(up_pre, approximate=True))
        return (hidden + jnp.einsum('bsf,fd->bsd', act_val, wd_f32)).astype(jnp.bfloat16)

    out_val, pullback = jax.vjp(
        forward,
        x_in.astype(jnp.float32),
        w_q.astype(jnp.float32),
        w_k.astype(jnp.float32),
        w_v.astype(jnp.float32),
        w_o.astype(jnp.float32),
        w_up.astype(jnp.float32),
        w_down.astype(jnp.float32),
    )
    grads = pullback(d_out)
    return (
        grads[0].astype(jnp.bfloat16),
        grads[1] / N_SHARDS,
        grads[2] / N_SHARDS,
        grads[3] / N_SHARDS,
        grads[4] / N_SHARDS,
        grads[5] / N_SHARDS,
        grads[6] / N_SHARDS,
    )
```

```python
import functools
import math

import jax
import jax.numpy as jnp
from jax import lax
from jax.experimental import pallas as pl
from jax.experimental.pallas import tpu as pltpu
from jax.sharding import PartitionSpec as P

BF16 = jnp.bfloat16
F32 = jnp.float32
NEG_BIG = -1e30
UNIT = 256
BLK = 256
GELU_C = math.sqrt(2.0 / math.pi)
GELU_A = 0.044715
LOG2E = math.log2(math.e)


def mm(a, b, ca, cb):
    return lax.dot_general(a, b, (((ca,), (cb,)), ((), ())), preferred_element_type=F32)


def gelu_parts(u):
    uu = u * u
    t = jnp.tanh(u * (GELU_C + (GELU_C * GELU_A) * uu))
    half = 0.5 * (1.0 + t)
    act = u * half
    der = half + (0.5 * u) * (1.0 - t * t) * (GELU_C + (3.0 * GELU_C * GELU_A) * uu)
    return act, der


def to_sequence(me, pieces, dst):
    for d, piece in enumerate(pieces):
        rank = jnp.bitwise_xor(me, d)
        lo = pl.multiple_of(rank * BLK, BLK)
        hi = pl.multiple_of((7 - rank) * BLK, BLK)
        dst[pl.ds(lo, BLK), :] = piece[0, :BLK, :]
        dst[pl.ds(hi, BLK), :] = piece[0, BLK:, :]


def from_sequence(me, src, pieces):
    for d, piece in enumerate(pieces):
        rank = jnp.bitwise_xor(me, d)
        lo = pl.multiple_of(rank * BLK, BLK)
        hi = pl.multiple_of((7 - rank) * BLK, BLK)
        piece[0, :BLK, :] = src[pl.ds(lo, BLK), :]
        piece[0, BLK:, :] = src[pl.ds(hi, BLK), :]


def diag_keep():
    key_pos = lax.broadcasted_iota(jnp.int32, (BLK, BLK), 0)
    query_pos = lax.broadcasted_iota(jnp.int32, (BLK, BLK), 1)
    return key_pos <= query_pos


def attn_fwd_kernel(scale, me_ref, *refs):
    q_in, k_in, v_in = refs[0:4], refs[4:8], refs[8:12]
    o_out, lse_out = refs[12:16], refs[16]
    qs, ks, vs, vt, os = refs[17:22]
    me = me_ref[0]
    to_sequence(me, q_in, qs)
    to_sequence(me, k_in, ks)
    to_sequence(me, v_in, vs)
    vt[...] = vs[...].T
    coef = scale * LOG2E
    for i in range(8):
        q_i = qs[i * BLK:(i + 1) * BLK, :]
        diag = mm(ks[i * BLK:(i + 1) * BLK, :], q_i, 1, 1)
        diag = jnp.where(diag_keep(), diag, NEG_BIG)
        top = jnp.max(diag, axis=0, keepdims=True)
        if i:
            past = mm(ks[:i * BLK, :], q_i, 1, 1)
            top = jnp.maximum(top, jnp.max(past, axis=0, keepdims=True))
        p_diag = jnp.exp2((diag - top) * coef)
        total = jnp.sum(p_diag, axis=0, keepdims=True)
        acc = mm(vt[:, i * BLK:(i + 1) * BLK], p_diag.astype(BF16), 1, 0)
        if i:
            p_past = jnp.exp2((past - top) * coef)
            total = total + jnp.sum(p_past, axis=0, keepdims=True)
            acc = acc + mm(vt[:, :i * BLK], p_past.astype(BF16), 1, 0)
        os[i * BLK:(i + 1) * BLK, :] = (acc / total).T.astype(BF16)
        lse_out[0, 0, i:i + 1, :] = top * coef + jnp.log2(total)
    from_sequence(me, os, o_out)


def attn_bwd_kernel(scale, me_ref, *refs):
    q_in, k_in, v_in, do_in, o_in = refs[0:4], refs[4:8], refs[8:12], refs[12:16], refs[16:20]
    lse_in = refs[20]
    gq_out, gk_out, gv_out = refs[21:25], refs[25:29], refs[29:33]
    qs, ks, vs, dos, kt, dsum, gqs, gks, gvs = refs[33:42]
    me = me_ref[0]
    to_sequence(me, q_in, qs)
    to_sequence(me, k_in, ks)
    to_sequence(me, v_in, vs)
    to_sequence(me, do_in, dos)
    kt[...] = ks[...].T
    for d in range(4):
        rank = jnp.bitwise_xor(me, d)
        prod = do_in[d][0].astype(F32) * o_in[d][0].astype(F32)
        sums = jnp.sum(prod.T, axis=0, keepdims=True)
        dsum[pl.ds(rank, 1), :] = sums[:, :BLK]
        dsum[pl.ds(7 - rank, 1), :] = sums[:, BLK:]
    coef = scale * LOG2E
    for i in range(8):
        here = slice(i * BLK, (i + 1) * BLK)
        q_i, do_i = qs[here, :], dos[here, :]
        lse_i, dot_i = lse_in[0, 0, i:i + 1, :], dsum[i:i + 1, :]
        gq = None
        for j in range(i + 1):
            at = slice(j * BLK, (j + 1) * BLK)
            prob = jnp.exp2(mm(ks[at, :], q_i, 1, 1) * coef - lse_i)
            if j == i:
                prob = jnp.where(diag_keep(), prob, 0.0)
            gp = mm(vs[at, :], do_i, 1, 1).astype(BF16).astype(F32)
            gs = (prob * (gp - dot_i) * scale).astype(BF16)
            gv = mm(prob.astype(BF16), do_i, 1, 0)
            gk = mm(gs, q_i, 1, 0)
            part = mm(kt[:, at], gs, 1, 0)
            gq = part if gq is None else gq + part
            if i == j:
                gks[at, :] = gk
                gvs[at, :] = gv
            else:
                gks[at, :] += gk
                gvs[at, :] += gv
        gqs[here, :] = gq.T
    for src, outs in ((gqs, gq_out), (gks, gk_out), (gvs, gv_out)):
        for d, piece in enumerate(outs):
            rank = jnp.bitwise_xor(me, d)
            lo = pl.multiple_of(rank * BLK, BLK)
            hi = pl.multiple_of((7 - rank) * BLK, BLK)
            piece[0, :BLK, :] = src[pl.ds(lo, BLK), :].astype(BF16)
            piece[0, BLK:, :] = src[pl.ds(hi, BLK), :].astype(BF16)


def attention_forward(me, qkv, heads):
    batch, seq, _ = qkv[0].shape
    full = 4 * seq

    def col(first):
        return pl.BlockSpec((1, seq, 128), lambda b, h, m: (b, 0, first + h))

    out = pl.pallas_call(
        functools.partial(attn_fwd_kernel, 128 ** -0.5),
        grid_spec=pltpu.PrefetchScalarGridSpec(
            num_scalar_prefetch=1, grid=(batch, heads),
            in_specs=[col(0)] * 4 + [col(heads)] * 4 + [col(2 * heads)] * 4,
            out_specs=[col(0)] * 4 + [pl.BlockSpec((1, 1, 8, BLK), lambda b, h, m: (b, h, 0, 0))],
            scratch_shapes=[pltpu.VMEM((full, 128), BF16), pltpu.VMEM((full, 128), BF16), pltpu.VMEM((full, 128), BF16),
                            pltpu.VMEM((128, full), BF16), pltpu.VMEM((full, 128), BF16)]),
        out_shape=[jax.ShapeDtypeStruct((batch, seq, heads * 128), BF16)] * 4
        + [jax.ShapeDtypeStruct((batch, heads, 8, BLK), F32)],
        compiler_params=pltpu.CompilerParams(vmem_limit_bytes=56 * 1024 * 1024),
        cost_estimate=pl.CostEstimate(flops=batch * heads * 36 * 4 * BLK * BLK * 256, bytes_accessed=batch * full * heads * 128 * 8,
                                      transcendentals=0),
        name="attn_fwd",
    )(me, *qkv, *qkv, *qkv)
    return out[:4], out[4]


def attention_backward(me, qkv, d_o, o, lse, heads):
    batch, seq, _ = qkv[0].shape
    full = 4 * seq

    def col(first):
        return pl.BlockSpec((1, seq, 128), lambda b, h, m: (b, 0, first + h))

    shape = jax.ShapeDtypeStruct((batch, seq, heads * 128), BF16)
    out = pl.pallas_call(
        functools.partial(attn_bwd_kernel, 128 ** -0.5),
        grid_spec=pltpu.PrefetchScalarGridSpec(
            num_scalar_prefetch=1, grid=(batch, heads),
            in_specs=[col(0)] * 4 + [col(heads)] * 4 + [col(2 * heads)] * 4 + [col(0)] * 8
            + [pl.BlockSpec((1, 1, 8, BLK), lambda b, h, m: (b, h, 0, 0))],
            out_specs=[col(0)] * 12,
            scratch_shapes=[pltpu.VMEM((full, 128), BF16)] * 4 + [pltpu.VMEM((128, full), BF16), pltpu.VMEM((8, BLK), F32)]
            + [pltpu.VMEM((full, 128), F32)] * 3),
        out_shape=[shape] * 12,
        compiler_params=pltpu.CompilerParams(vmem_limit_bytes=56 * 1024 * 1024),
        cost_estimate=pl.CostEstimate(flops=batch * heads * 36 * 10 * BLK * BLK * 256, bytes_accessed=batch * full * heads * 128 * 16,
                                      transcendentals=0),
        name="attn_bwd",
    )(me, *qkv, *qkv, *qkv, *d_o, *o, lse)
    return out[0:4], out[4:8], out[8:12]


def chain_kernel(rows, h_ref, d_ref, w_ref, ga_ref, out_ref, acc):
    step = pl.program_id(0)
    for r in range(h_ref.shape[0] // rows):
        at = slice(r * rows, (r + 1) * rows)
        u = mm(h_ref[at, :], w_ref[...], 1, 0).astype(BF16).astype(F32)
        _, der = gelu_parts(u)
        gp = (ga_ref[at, :].astype(F32) * der).astype(BF16)
        part = mm(gp, w_ref[...], 1, 1)

        @pl.when(step == 0)
        def _():
            acc[at, :] = part

        @pl.when(step > 0)
        def _():
            acc[at, :] += part

    @pl.when(step == pl.num_programs(0) - 1)
    def _():
        out_ref[...] = (d_ref[...].astype(F32) + acc[...]).astype(BF16)


def hidden_chain(hidden, d_out, w_up, grad_act):
    n, dim = hidden.shape
    ffn = w_up.shape[1]
    cols = 5 * UNIT
    return pl.pallas_call(
        functools.partial(chain_kernel, 512),
        grid=(ffn // cols,),
        in_specs=[pl.BlockSpec((n, dim), lambda f: (0, 0)), pl.BlockSpec((n, dim), lambda f: (0, 0)),
                  pl.BlockSpec((dim, cols), lambda f: (0, f)), pl.BlockSpec((n, cols), lambda f: (0, f))],
        out_specs=pl.BlockSpec((n, dim), lambda f: (0, 0)),
        out_shape=jax.ShapeDtypeStruct((n, dim), BF16),
        scratch_shapes=[pltpu.VMEM((n, dim), F32)],
        compiler_params=pltpu.CompilerParams(vmem_limit_bytes=62 * 1024 * 1024),
        cost_estimate=pl.CostEstimate(flops=4 * n * dim * ffn, bytes_accessed=2 * (n + dim) * ffn, transcendentals=0),
        name="hidden_chain",
    )(hidden, d_out, w_up, grad_act)


def wgrad_kernel(n_piece, n_batch, with_in, *refs):
    h_in, d_in = refs[0:n_piece], refs[n_piece:2 * n_piece]
    refs = refs[2 * n_piece:]
    wu_ref, wd_ref = refs[0:2]
    refs = refs[2:]
    if with_in:
        gd_in, gu_in = refs[0:2]
        refs = refs[2:]
    gd_ref, gu_ref, h_buf, d_buf, sems = refs[0:5]
    if with_in:
        gd_buf, gu_buf, in_sems = refs[5:8]
    f, t = pl.program_id(0), pl.program_id(1)
    n_t = n_piece * n_batch
    steps = pl.num_programs(0) * n_t
    step = f * n_t + t
    slot = lax.rem(step, 2)

    def copies(piece, batch, to):
        return (pltpu.make_async_copy(h_in[piece].at[batch], h_buf.at[to], sems.at[0, to]),
                pltpu.make_async_copy(d_in[piece].at[batch], d_buf.at[to], sems.at[1, to]))

    def fetch(at, to):
        for piece in range(n_piece):
            @pl.when(at // n_batch == piece)
            def _():
                for copy in copies(piece, lax.rem(at, n_batch), to):
                    copy.start()

    def in_copies():
        size = gd_ref.shape[0]
        row = pl.multiple_of(f * size, size)
        return (pltpu.make_async_copy(gd_in.at[pl.ds(row, size)], gd_buf, in_sems.at[0]),
                pltpu.make_async_copy(gu_in.at[pl.ds(row, size)], gu_buf, in_sems.at[1]))

    @pl.when(step == 0)
    def _():
        fetch(0, 0)

    @pl.when(step + 1 < steps)
    def _():
        fetch(lax.rem(t + 1, n_t), 1 - slot)

    if with_in:
        @pl.when(t == 0)
        def _():
            for copy in in_copies():
                copy.start()

    for copy in copies(0, 0, slot):
        copy.wait()
    h, d = h_buf[slot], d_buf[slot]
    u = mm(h, wu_ref[...], 1, 0).astype(BF16).astype(F32)
    ga = mm(d, wd_ref[...], 1, 0).astype(BF16).astype(F32)
    act, der = gelu_parts(u)
    gp = (ga * der).astype(BF16)
    gd = mm(act.astype(BF16), d, 0, 0)
    gu = mm(gp, h, 0, 0)

    @pl.when(t == 0)
    def _():
        gd_ref[...] = gd
        gu_ref[...] = gu

    @pl.when(t > 0)
    def _():
        gd_ref[...] += gd
        gu_ref[...] += gu

    if with_in:
        @pl.when(t == n_t - 1)
        def _():
            for copy in in_copies():
                copy.wait()
            gd_ref[...] += gd_buf[...]
            gu_ref[...] += gu_buf[...]


def ffn_wgrad(hidden, d_out, w_up_t, w_down_t, cols, block, start=None):
    n_piece = len(hidden)
    n_batch, seq, dim = hidden[0].shape
    n_f = cols // block
    hbm = pl.BlockSpec(memory_space=pl.ANY)
    once = {} if n_f > 1 else {"pipeline_mode": pl.Buffered(1)}
    w_spec = pl.BlockSpec((dim, block), lambda f, t: (0, f), **once)
    o_spec = pl.BlockSpec((block, dim), lambda f, t: (f, 0))
    extra = () if start is None else tuple(start)
    scratch = [pltpu.VMEM((2, seq, dim), BF16), pltpu.VMEM((2, seq, dim), BF16), pltpu.SemaphoreType.DMA((2, 2))]
    if start is not None:
        scratch += [pltpu.VMEM((block, dim), F32), pltpu.VMEM((block, dim), F32), pltpu.SemaphoreType.DMA((2,))]
    tokens = n_piece * n_batch * seq
    return pl.pallas_call(
        functools.partial(wgrad_kernel, n_piece, n_batch, start is not None),
        grid=(n_f, n_piece * n_batch),
        in_specs=[hbm] * (2 * n_piece) + [w_spec, w_spec] + [hbm] * len(extra),
        out_specs=[o_spec, o_spec],
        out_shape=[jax.ShapeDtypeStruct((cols, dim), F32)] * 2,
        scratch_shapes=scratch,
        compiler_params=pltpu.CompilerParams(vmem_limit_bytes=63 * 1024 * 1024),
        cost_estimate=pl.CostEstimate(flops=8 * tokens * dim * cols, bytes_accessed=4 * tokens * dim * n_f + 16 * cols * dim,
                                      transcendentals=0),
        name="ffn_wgrad",
    )(*hidden, *d_out, w_up_t, w_down_t, *extra)


def place_kernel(per, n_src, factor, *refs):
    srcs, out_ref = refs[1:1 + n_src], refs[-1]
    i = pl.program_id(0)
    for k in range(n_src):
        @pl.when(i // per == k)
        def _():
            value = srcs[k][...] * factor
            out_ref[...] = value.T if out_ref.shape != value.shape else value


def place(first_unit, chunks, target, shape, transpose, factor):
    n_src = len(chunks)
    rows, dim = chunks[0].shape
    per = rows // UNIT

    def src_spec(k):
        return pl.BlockSpec((UNIT, dim), lambda i, u: (jnp.clip(i - k * per, 0, per - 1), 0))

    if transpose:
        out_spec = pl.BlockSpec((dim, UNIT), lambda i, u: (0, u[0] + i))
    else:
        out_spec = pl.BlockSpec((UNIT, dim), lambda i, u: (u[0] + i, 0))
    extra = () if target is None else (target,)
    return pl.pallas_call(
        functools.partial(place_kernel, per, n_src, factor),
        grid_spec=pltpu.PrefetchScalarGridSpec(
            num_scalar_prefetch=1, grid=(n_src * per,),
            in_specs=[src_spec(k) for k in range(n_src)] + [pl.BlockSpec(memory_space=pl.ANY)] * len(extra),
            out_specs=out_spec),
        out_shape=jax.ShapeDtypeStruct(shape, F32),
        input_output_aliases={} if target is None else {1 + n_src: 0},
        compiler_params=pltpu.CompilerParams(vmem_limit_bytes=56 * 1024 * 1024),
        cost_estimate=pl.CostEstimate(flops=n_src * rows * dim * 60, bytes_accessed=8 * n_src * rows * dim, transcendentals=0),
        name="place_t" if transpose else "place",
    )(first_unit, *chunks, *extra)


def solution(mesh):
    cp_size = mesh.shape['cp']
    n_total = mesh.shape['dp'] * cp_size
    assert cp_size == 4 and mesh.shape['dp'] == 2

    def swap(flip):
        pairs = [(rank, rank ^ flip) for rank in range(cp_size)]
        return lambda value: lax.ppermute(value, 'cp', pairs)

    to_core, to_x, to_xc = swap(1), swap(2), swap(3)

    def to_y(value):
        return lax.ppermute(value, 'dp', [(0, 1), (1, 0)])

    def after(value, *earlier):
        return lax.optimization_barrier((value,) + earlier)[0]

    def per_device(x_in, d_out, w_q, w_k, w_v, w_o, w_up, w_down):
        me = lax.axis_index('cp')
        row = lax.axis_index('dp')
        core = lax.rem(me, 2)
        parity = lax.rem(me // 2 + row, 2)
        me_vec = jnp.full((1,), me, jnp.int32)
        batch, seq, dim = x_in.shape
        n_heads, head_dim = w_q.shape[1], w_q.shape[2]
        heads = n_heads // cp_size
        width = heads * head_dim
        ffn = w_up.shape[1]
        tokens = batch * seq
        flat = lambda a: a.reshape(tokens, a.shape[-1])

        x_x = to_x(x_in)
        x_c = to_core(x_in)
        x_xc = to_core(x_x)
        xs = [x_in, x_c, x_x, x_xc]

        wt = [w.transpose(1, 0, 2) for w in (w_q, w_k, w_v)]
        w_heads = []
        for d in range(4):
            first = heads * jnp.bitwise_xor(me, d)
            parts = [lax.dynamic_slice_in_dim(w, first, heads, 0) for w in wt]
            w_heads.append(jnp.concatenate(parts, 0).transpose(1, 0, 2).reshape(dim, 3 * width))
        wo_flat = w_o.reshape(n_heads * head_dim, dim)
        wo_heads = [lax.dynamic_slice_in_dim(wo_flat, width * jnp.bitwise_xor(me, d), width, 0) for d in range(4)]

        grad_act = mm(flat(d_out), w_down, 1, 1).astype(BF16)

        qkv = [mm(flat(x), w_heads[0], 1, 0).astype(BF16).reshape(batch, seq, 3 * width) for x in xs]
        o, lse = attention_forward(me_vec, qkv, heads)

        o_x = [to_x(o[d ^ 2]) for d in range(4)]
        o_c = {d: to_core(o[d ^ 1]) for d in (0, 2)}
        o_xc = {d: to_core(o_x[d ^ 1]) for d in (0, 2)}
        wo_all = jnp.concatenate(wo_heads, 0)

        def hidden_of(d):
            o_all = jnp.concatenate([flat(o[d]), flat(o_c[d]), flat(o_x[d]), flat(o_xc[d])], 1)
            return (flat(xs[d]).astype(F32) + mm(o_all, wo_all, 1, 0)).astype(BF16).reshape(batch, seq, dim)

        h_own, h_x = hidden_of(0), hidden_of(2)
        h_c, h_xc = to_core(h_own), to_core(h_x)
        hs = [h_own, h_c, h_x, h_xc]

        d_y = to_y(d_out)
        d_x = to_x(after(d_out, x_x))
        d_yx = to_y(d_x)
        ds = [d_out, to_core(d_out), d_x, to_core(d_x)]
        ds_y = [d_y, to_core(d_y), d_yx, to_core(d_yx)]
        h_y, h_yx = to_y(h_own), to_y(h_x)
        hs_y = [h_y, to_core(h_y), h_yx, to_core(h_yx)]

        gh = hidden_chain(flat(h_own), flat(d_out), w_up, grad_act).reshape(batch, seq, dim)
        gh_x = to_x(gh)
        gh_c = to_core(gh)
        gh_xc = to_core(gh_x)
        ghs = [gh, gh_c, gh_x, gh_xc]

        units = 9
        starts = jnp.array([0, 9, 17, 26], jnp.int32)
        slot_start = lambda par, cor: starts[2 * par + cor]
        first = slot_start(parity, core)
        cols = units * UNIT
        wu_mine = lax.dynamic_slice(w_up, (0, first * UNIT), (dim, cols))
        wd_mine = lax.dynamic_slice(w_down, (first * UNIT, 0), (cols, dim)).T
        chunk = 3 * UNIT
        hs_a = [after(h, gh) for h in hs]
        part = ffn_wgrad(hs_a, ds, wu_mine, wd_mine, cols, chunk)

        d_o = [mm(flat(after(g, part[0])), wo_heads[0], 1, 1).astype(BF16).reshape(batch, seq, width) for g in ghs]
        gq, gk, gv = attention_backward(me_vec, qkv, d_o, o, lse, heads)
        g_all = [jnp.concatenate([gq[d], gk[d], gv[d]], -1) for d in range(4)]
        g_c, g_x, g_xc = to_core(g_all[1]), to_x(g_all[2]), to_xc(g_all[3])

        gw_qkv = sum(mm(flat(xs[d]), flat(g_all[d]), 0, 0) for d in range(4))
        gw_o = sum(mm(flat(o[d]), flat(ghs[d]), 0, 0) for d in range(4))

        sent = []
        order = gw_qkv
        for k in range(cols // chunk):
            at = slice(k * chunk, (k + 1) * chunk)
            hs_b = [after(hs_y[0], order)] + hs_y[1:]
            done = ffn_wgrad(hs_b, ds_y, wu_mine[:, at], wd_mine[:, at], chunk, chunk, start=(part[0][at], part[1][at]))
            order = done[0]
            sent.append(done)

        gw_qkv = gw_qkv + to_y(gw_qkv)
        gw_o = gw_o + to_y(gw_o)

        scale = 1.0 / n_total
        down = {(0, 0): [s[0] for s in sent]}
        up = {(0, 0): [s[1] for s in sent]}
        down[1, 0] = [to_x(s) for s in down[0, 0]]
        up[1, 0] = [to_y(s) for s in up[0, 0]]
        g_down = g_up = None
        for par in range(2):
            down[par, 1] = [to_core(s) for s in down[par, 0]]
            up[par, 1] = [to_core(s) for s in up[par, 0]]
        for par in range(2):
            for cor in range(2):
                unit = slot_start(jnp.bitwise_xor(parity, par), jnp.bitwise_xor(core, cor)).reshape(1)
                g_down = place(unit, down[par, cor], g_down, (ffn, dim), False, scale)
                g_up = place(unit, up[par, cor], g_up, (dim, ffn), True, scale)

        def gather_heads(mine):
            x_part = to_x(mine)
            return [mine, to_core(mine), x_part, to_core(x_part)]

        gqkv_parts = gather_heads(gw_qkv)
        go_parts = gather_heads(gw_o)
        outs = []
        for n in range(3):
            total = jnp.zeros((n_heads, dim, head_dim), F32)
            for d in range(4):
                slab = gqkv_parts[d][:, n * width:(n + 1) * width].reshape(dim, heads, head_dim).transpose(1, 0, 2) * scale
                total = lax.dynamic_update_slice(total, slab, (heads * jnp.bitwise_xor(me, d), 0, 0))
            outs.append(total.transpose(1, 0, 2))
        g_o = jnp.zeros((n_heads * head_dim, dim), F32)
        for d in range(4):
            g_o = lax.dynamic_update_slice(g_o, go_parts[d] * scale, (width * jnp.bitwise_xor(me, d), 0))
        g_o = g_o.reshape(n_heads, head_dim, dim)

        total = gh.reshape(tokens, dim).astype(F32)
        for d, g in enumerate((g_all[0], g_c, g_x, g_xc)):
            total = total + mm(flat(g), w_heads[d], 1, 1)
        grad_x = total.astype(BF16).reshape(batch, seq, dim)
        return (grad_x, *outs, g_o, g_up, g_down)

    act_spec = P('dp', 'cp', None)
    return jax.shard_map(per_device, mesh=mesh,
                         in_specs=(act_spec, act_spec, P(), P(), P(), P(), P(), P()),
                         out_specs=(act_spec, P(), P(), P(), P(), P(), P()),
                         check_vma=False)
```
